16 devices in a mesh: dp: 4 (over y, z, core), ep: 4 (over x).
Axes of the slice: x: 4, y: 2, z: 1, core: 2. Of those that a mesh axis runs over, the one named last changes fastest.
The devices are a block of a 4x4x8 slice.
Arguments:
- x: bfloat16 [4, 4, 512, 2048], P('dp', 'ep'), parts along dimension 0
- expert: int32 [4, 4, 512, 8], P('dp', 'ep'), parts along dimension 0
- slot: int32 [4, 4, 512, 8], P('dp', 'ep'), parts along dimension 0
- gate: float32 [4, 4, 512, 8], P('dp', 'ep'), parts along dimension 0
- w_gate: bfloat16 [64, 2048, 1024], P('ep')
- w_up: bfloat16 [64, 2048, 1024], P('ep')
- w_down: bfloat16 [64, 1024, 2048], P('ep')
Outputs:
- y: bfloat16 [4, 4, 512, 2048], P('dp', 'ep'), parts along dimension 0
There are 4 independent parts. The reference program is written for one: setup_inputs(seed, part) draws one part's arguments, and reference() takes and returns one part's arrays. A program takes and returns all parts, laid end to end along the dimension named above; an argument that names none is the same for every part.
All inputs are finite; a program needn't handle non-finite values.
Results may differ from the reference program's by a relative error of at most 0.009.
Values are sent between devices in bfloat16 or wider.
A program may use at most 768 MiB of HBM per device.

```python
import jax
import jax.numpy as jnp

MEMBERS = 4
TOKENS = 512
D = 2048
FF = 1024
TOP = 8
EXPERTS = 64
SLOTS = 5 * TOKENS * TOP // (4 * EXPERTS)


def setup_inputs(seed: int = 0, part: int = 0) -> dict:
    own, k1, k2, k3, k4, k5, k6 = jax.random.split(jax.random.key(seed), 7)
    kx, ke, kl, kg = jax.random.split(jax.random.fold_in(own, part), 4)
    devices = (1, MEMBERS)
    place = jax.random.permutation(kl, jnp.arange(EXPERTS, dtype=jnp.uint32))
    slow = ((EXPERTS + (9 * place) % EXPERTS) << ((9 * place) // EXPERTS)) // EXPERTS
    wait = (jax.random.bits(ke, (*devices, TOKENS, EXPERTS), jnp.uint32) >> 10) * slow
    expert = jnp.argsort(wait, axis=-1)[..., :TOP].astype(jnp.int32)
    chosen = jax.nn.one_hot(expert, EXPERTS, dtype=jnp.int32)
    in_line = jnp.cumsum(chosen.reshape(*devices, TOKENS * TOP, EXPERTS), axis=2) - 1
    slot = jnp.sum(in_line.reshape(chosen.shape) * chosen, axis=-1)

    def one(key, rows, columns):
        return (jax.random.normal(key, (rows, columns), jnp.float32) * rows**-0.5).astype(jnp.bfloat16)

    def weights(key, rows, columns):
        return jax.lax.map(lambda k: one(k, rows, columns), jax.random.split(key, EXPERTS))

    return {
        "x": jax.random.normal(kx, (*devices, TOKENS, D), jnp.float32).astype(jnp.bfloat16),
        "expert": expert,
        "slot": slot,
        "gate": jax.nn.softmax(jax.random.normal(kg, expert.shape, jnp.float32)),
        "w_gate": weights(k1, D, FF),
        "w_up": weights(k2, D, FF),
        "w_down": weights(k3, FF, D),
    }


def einsum(form, a, b):
    return jnp.einsum(form, a.astype(jnp.float32), b.astype(jnp.float32))


def reference(x, expert, slot, gate, w_gate, w_up, w_down):
    to_expert = jax.nn.one_hot(expert, EXPERTS, dtype=jnp.bfloat16)
    to_slot = jax.nn.one_hot(slot, SLOTS, dtype=jnp.bfloat16)
    weighted = to_expert * gate[..., None].astype(jnp.bfloat16)
    dispatch = einsum("abtke,abtkc->abtec", to_expert, to_slot).astype(jnp.bfloat16)
    combine = einsum("abtke,abtkc->abtec", weighted, to_slot).astype(jnp.bfloat16)
    z = einsum("abtec,abtd->aebcd", dispatch, x).astype(jnp.bfloat16)
    h = jax.nn.silu(einsum("aebcd,edf->aebcf", z, w_gate))
    h = (h * einsum("aebcd,edf->aebcf", z, w_up)).astype(jnp.bfloat16)
    out = einsum("aebcf,efd->aebcd", h, w_down).astype(jnp.bfloat16)
    y = einsum("abtec,aebcd->abtd", combine, out)
    return y.astype(jnp.bfloat16)
```

```python
import functools

import jax
import jax.numpy as jnp
from jax import lax
from jax.experimental import pallas as pl
from jax.experimental.pallas import tpu as pltpu
from jax.sharding import PartitionSpec as P

BF = jnp.bfloat16
F32 = jnp.float32
BC = 256
NB = 8


def dot(a, b):
    return jnp.dot(a, b, preferred_element_type=F32)


def kernel(
    n, el, cap, x_ref, meta_ref, wg_ref, wu_ref, wd_ref,
    y_ref, xg_ref, ro_ref, rl_ref,
    acc_g, acc_u, dmat, wmat, xbuf, zbuf, wbuf, so_buf, sl_buf, st_o, st_l, ybuf, meta, sg,
    wsem, xsem, xs_send, xs_recv, m_send, m_recv, o_send, o_recv, l_send, l_recv, st_sem, y_sem,
):
    tokens, d = x_ref.shape
    ff = wg_ref.shape[2]
    nc = d // BC
    half = tokens // 2
    rows = n * cap
    per = el * cap
    me = lax.axis_index("ep")
    right, left, opp = lax.rem(me + 1, n), lax.rem(me + n - 1, n), lax.rem(me + 2, n)
    tiles1 = nc * el * 2
    tiles = tiles1 + nc * el


    def start_gu(c, e, which):
        q = c * (2 * el) + 2 * e + which
        s = lax.rem(q, NB)
        w = (wg_ref, wu_ref)[which]
        for j in range(ff // BC):
            pltpu.make_async_copy(
                w.at[e, pl.ds(c * BC, BC), pl.ds(j * BC, BC)], wbuf.at[s, pl.ds(j * BC, BC)], wsem.at[s]
            ).start()

    def start_dn(c, e):
        s = lax.rem(tiles1 + c * el + e, NB)
        pltpu.make_async_copy(wd_ref.at[e, :, pl.ds(c * BC, BC)], wbuf.at[s], wsem.at[s]).start()

    def start_tile(q, which):
        @pl.when(q < tiles1)
        def _():
            c = q // (2 * el)
            start_gu(c, lax.rem(q, 2 * el) // 2, which)

        @pl.when(jnp.logical_and(q >= tiles1, q < tiles))
        def _():
            r = q - tiles1
            start_dn(r // el, lax.rem(r, el))

    def wait_tile(q):
        s = lax.rem(q, NB)
        pltpu.make_async_copy(wbuf.at[s], wbuf.at[s], wsem.at[s]).wait()
        return s

    for q in range(NB):
        start_tile(q, q % 2)

    def load_own(c):
        return pltpu.make_async_copy(x_ref.at[:, pl.ds(c * BC, BC)], xbuf.at[lax.rem(c, 2), 0], xsem.at[0])

    load_own(0).start()

    def send(src, dst, ss, rs, to):
        return pltpu.make_async_remote_copy(
            src_ref=src, dst_ref=dst, send_sem=ss, recv_sem=rs, device_id={"ep": to},
            device_id_type=pl.DeviceIdType.MESH,
        )

    def own(c, direction, part):
        h = part if direction == 0 else 1 - part
        i = 2 * direction + part
        return send(
            x_ref.at[pl.ds(h * half, half), pl.ds(c * BC, BC)],
            xg_ref.at[direction, c, pl.ds(h * half, half)],
            xs_send.at[i, c], xs_recv.at[i, c], (right, left)[direction],
        )

    def forward(c, direction):
        h = direction
        return send(
            xg_ref.at[direction, c, pl.ds(h * half, half)],
            xg_ref.at[2, c, pl.ds(h * half, half)],
            xs_send.at[4 + direction, c], xs_recv.at[4 + direction, c], (right, left)[direction],
        )

    def service(c):
        @pl.when(c < nc)
        def _():
            for direction in range(2):
                own(c, direction, 0).wait_recv()
                forward(c, direction).start()

        @pl.when(c + 1 < nc)
        def _():
            for direction in range(2):
                own(c + 1, direction, 1).start()

        @pl.when(c + 2 < nc)
        def _():
            for direction in range(2):
                own(c + 2, direction, 0).start()

    barrier = pltpu.get_barrier_semaphore()
    for to in (left, right, opp):
        pl.semaphore_signal(barrier, inc=1, device_id={"ep": to}, device_id_type=pl.DeviceIdType.MESH)
    pl.semaphore_wait(barrier, 3)

    metas = [
        send(meta_ref, meta.at[1 + i], m_send.at[i], m_recv.at[i], to) for i, to in enumerate((right, left, opp))
    ]
    for m in metas:
        m.start()
    for direction in range(2):
        own(0, direction, 0).start()
    for direction in range(2):
        own(0, direction, 1).start()
    if nc > 1:
        for direction in range(2):
            own(1, direction, 0).start()

    def clear(i, _):
        acc_g[i] = jnp.zeros(acc_g.shape[1:], F32)
        acc_u[i] = jnp.zeros(acc_u.shape[1:], F32)
        return 0

    meta[0] = meta_ref[...]
    lax.fori_loop(0, el, clear, 0)

    top = meta_ref.shape[0] // 2
    base = (me * per).astype(F32)
    first = lax.broadcasted_iota(jnp.int32, (el, tokens), 0).astype(F32) * cap + base
    line = lax.broadcasted_iota(jnp.int32, (cap, tokens), 0).astype(F32)

    def build(b, _):
        @pl.when(b == 1)
        def _():
            for m in metas:
                m.wait_recv()

        s = jnp.full((el, tokens), -1.0, F32)
        g = jnp.zeros((el, tokens), F32)
        for k in range(top):
            r = meta[b, pl.ds(k, 1)] - first
            ok = jnp.logical_and(r >= 0.0, r < cap)
            s = jnp.where(ok, r, s)
            g = jnp.where(ok, meta[b, pl.ds(top + k, 1)], g)
        sg[0] = s
        sg[1] = g

        def lines(e, _):
            eq = sg[0, pl.ds(e, 1)] == line
            at = pl.multiple_of(e * cap, 16)
            dmat[b, pl.ds(at, cap)] = jnp.where(eq, 1.0, 0.0).astype(BF)
            w = jnp.where(eq, sg[1, pl.ds(e, 1)], 0.0).astype(BF)
            for j in range(tokens // BC):
                zbuf[pl.ds(pl.multiple_of(j * per + e * cap, 16), cap)] = w[:, j * BC : (j + 1) * BC]
            return 0

        lax.fori_loop(0, el, lines, 0)
        for i in range(per // 128):
            for j in range(tokens // BC):
                t = zbuf[pl.ds(j * per + i * 128, 128)]
                wmat[b, pl.ds(j * BC, BC), pl.ds(i * 128, 128)] = t.T
        return 0

    lax.fori_loop(0, n, build, 0)
    service(0)

    def gate_up(c, p, last):
        for u in range(2):
            e = 2 * p + u
            q = c * (2 * el) + 2 * e
            z = zbuf[pl.ds(pl.multiple_of(e * rows, 16), rows)]
            sa = wait_tile(q)
            sb = wait_tile(q + 1)
            for j in range(ff // BC):
                cols = pl.ds(j * BC, BC)
                g = acc_g[e, :, cols] + dot(z, wbuf[sa, cols])
                v = acc_u[e, :, cols] + dot(z, wbuf[sb, cols])
                if last:
                    acc_g[e, :, cols] = (g * jax.nn.sigmoid(g) * v).astype(BF).astype(F32)
                else:
                    acc_g[e, :, cols] = g
                    acc_u[e, :, cols] = v
            start_tile(q + NB, 0)
            start_tile(q + NB + 1, 1)

    def phase1(c, last):
        slot = lax.rem(c, 2)
        for direction in range(2):
            own(c, direction, 1).wait_recv()
        loads = [
            pltpu.make_async_copy(xg_ref.at[i, c], xbuf.at[slot, 1 + i], xsem.at[1 + i]) for i in range(3)
        ]
        loads[0].start()
        loads[1].start()
        for direction in range(2):
            forward(c, direction).wait_recv()
        loads[2].start()
        for b in range(n):
            if b == 0:
                load_own(c).wait()
            else:
                loads[b - 1].wait()
            z = dot(dmat[b], xbuf[slot, b]).astype(BF)
            for e in range(el):
                zbuf[pl.ds(e * rows + b * cap, cap)] = z[e * cap : (e + 1) * cap]
        if not last:
            load_own(c + 1).start()

        def body(p, _):
            gate_up(c, p, last)
            return 0

        lax.fori_loop(0, el // 4, body, 0)
        if not last:
            service(c + 1)
        lax.fori_loop(el // 4, el // 2, body, 0)

    def loop1(c, _):
        phase1(c, False)
        return 0

    lax.fori_loop(0, nc - 1, loop1, 0)
    phase1(nc - 1, True)

    def keep(kind, c, value):
        for i in range(2):
            acc_u[2 * c + i, pl.ds(0, half), pl.ds(kind * BC, BC)] = value[i * half : (i + 1) * half]

    def kept(kind, c, i):
        return acc_u[2 * c + i, pl.ds(0, half), pl.ds(kind * BC, BC)]

    def send_o(c, i):
        slot = lax.rem(c, 2)
        return send(
            so_buf.at[slot, pl.ds(i * half, half)], ro_ref.at[c, i], o_send.at[i, slot], o_recv.at[i, c],
            (left, right)[i],
        )

    def send_l(c, i):
        slot = lax.rem(c, 2)
        return send(
            sl_buf.at[slot, i], rl_ref.at[c, i], l_send.at[i, slot], l_recv.at[i, c], (left, right)[i]
        )

    def stage_o(c):
        return pltpu.make_async_copy(ro_ref.at[c], st_o, st_sem.at[0])

    def stage_l(c):
        return pltpu.make_async_copy(rl_ref.at[c], st_l, st_sem.at[1])

    def out_y(c):
        slot = lax.rem(c, 2)
        return pltpu.make_async_copy(ybuf.at[slot], y_ref.at[:, pl.ds(c * BC, BC)], y_sem.at[slot])

    def arrive_o(c):
        for i in range(2):
            send_o(c, i).wait_recv()
        stage_o(c).start()

    def arrive_l(c):
        for i in range(2):
            send_l(c, i).wait_recv()
        stage_l(c).start()

    def pass_on(c):
        stage_o(c).wait()
        slot = lax.rem(c, 2)

        @pl.when(c >= 2)
        def _():
            for i in range(2):
                send_l(c - 2, i).wait_send()

        for i in range(2):
            sl_buf[slot, i, pl.ds(i * half, half)] = (kept(1 + i, c, i) + st_o[i].astype(F32)).astype(BF)
            sl_buf[slot, i, pl.ds((1 - i) * half, half)] = kept(1 + i, c, 1 - i).astype(BF)
            send_l(c, i).start()

    def finish(c):
        stage_l(c).wait()
        slot = lax.rem(c, 2)

        @pl.when(c >= 2)
        def _():
            out_y(c - 2).wait()

        for i in range(2):
            r = pl.ds(i * half, half)
            ybuf[slot, r] = (kept(0, c, i) + st_l[0, r].astype(F32) + st_l[1, r].astype(F32)).astype(BF)
        out_y(c).start()

    def phase2(c, _):
        def down(p, _):
            for u in range(2):
                e = 2 * p + u
                q = tiles1 + c * el + e
                s = wait_tile(q)
                o = dot(acc_g[e].astype(BF), wbuf[s]).astype(BF)
                for b in range(n):
                    zbuf[pl.ds(pl.multiple_of(b * per + e * cap, 16), cap)] = o[b * cap : (b + 1) * cap]
                start_tile(q + NB, u)
            return 0

        lax.fori_loop(0, el // 4, down, 0)

        @pl.when(c >= 1)
        def _():
            arrive_o(c - 1)

        @pl.when(c >= 2)
        def _():
            arrive_l(c - 2)

        lax.fori_loop(el // 4, el // 2, down, 0)

        slot = lax.rem(c, 2)

        @pl.when(c >= 2)
        def _():
            for i in range(2):
                send_o(c - 2, i).wait_send()

        so_buf[slot] = dot(wmat[3], zbuf[pl.ds(3 * per, per)]).astype(BF)
        for i in range(2):
            send_o(c, i).start()

        @pl.when(c >= 1)
        def _():
            pass_on(c - 1)

        for kind in range(3):
            keep(kind, c, dot(wmat[kind], zbuf[pl.ds(kind * per, per)]))

        @pl.when(c >= 2)
        def _():
            finish(c - 2)

        return 0

    lax.fori_loop(0, nc, phase2, 0)
    arrive_o(nc - 1)
    pass_on(nc - 1)
    for c in (nc - 2, nc - 1):
        arrive_l(c)
        finish(c)
    for c in (nc - 2, nc - 1):
        out_y(c).wait()
        for i in range(2):
            send_o(c, i).wait_send()
            send_l(c, i).wait_send()

    def drain(c, _):
        for direction in range(2):
            for part in range(2):
                own(c, direction, part).wait_send()
            forward(c, direction).wait_send()
        return 0

    lax.fori_loop(0, nc, drain, 0)
    for m in metas:
        m.wait_send()


def solution(mesh):
    n = mesh.shape["ep"]

    def step(x, expert, slot, gate, w_gate, w_up, w_down):
        x, expert, slot, gate = (v[0, 0] for v in (x, expert, slot, gate))
        tokens, d = x.shape
        el, _, ff = w_gate.shape
        top = expert.shape[1]
        cap = 5 * tokens * top // (4 * el * n)
        nc = d // BC
        half = tokens // 2
        key = jnp.where(slot < cap, expert * cap + slot, -1)
        meta = jnp.concatenate([key.astype(F32).T, gate.astype(BF).astype(F32).T], 0)
        any_, vmem = pl.BlockSpec(memory_space=pl.ANY), pl.BlockSpec(memory_space=pltpu.VMEM)
        dma = pltpu.SemaphoreType.DMA
        y, *_ = pl.pallas_call(
            functools.partial(kernel, n, el, cap),
            out_shape=[
                jax.ShapeDtypeStruct((tokens, d), BF),
                jax.ShapeDtypeStruct((n - 1, nc, tokens, BC), BF),
                jax.ShapeDtypeStruct((nc, 2, half, BC), BF),
                jax.ShapeDtypeStruct((nc, 2, tokens, BC), BF),
            ],
            in_specs=[any_, vmem, any_, any_, any_],
            out_specs=[any_] * 4,
            scratch_shapes=[
                pltpu.VMEM((el, n * cap, ff), F32),
                pltpu.VMEM((el, n * cap, ff), F32),
                pltpu.VMEM((n, el * cap, tokens), BF),
                pltpu.VMEM((n, tokens, el * cap), BF),
                pltpu.VMEM((2, n, tokens, BC), BF),
                pltpu.VMEM((n * el * cap, BC), BF),
                pltpu.VMEM((NB, ff, BC), BF),
                pltpu.VMEM((2, tokens, BC), BF),
                pltpu.VMEM((2, 2, tokens, BC), BF),
                pltpu.VMEM((2, half, BC), BF),
                pltpu.VMEM((2, tokens, BC), BF),
                pltpu.VMEM((2, tokens, BC), BF),
                pltpu.VMEM((n, 2 * top, tokens), F32),
                pltpu.VMEM((2, el, tokens), F32),
                dma((NB,)),
                dma((n,)),
                dma((6, nc)),
                dma((6, nc)),
                dma((3,)),
                dma((3,)),
                dma((2, 2)),
                dma((2, nc)),
                dma((2, 2)),
                dma((2, nc)),
                dma((2,)),
                dma((2,)),
            ],
            compiler_params=pltpu.CompilerParams(
                collective_id=0, has_side_effects=True, vmem_limit_bytes=67043328
            ),
        )(x, meta, w_gate, w_up, w_down)
        return y[None, None]

    token, weight = P("dp", "ep", None, None), P("ep", None, None)
    return jax.shard_map(
        step,
        mesh=mesh,
        in_specs=(token,) * 4 + (weight,) * 3,
        out_specs=token,
        check_vma=False,
    )
```

```python
import functools

import jax
import jax.numpy as jnp
from jax import lax
from jax.experimental import pallas as pl
from jax.experimental.pallas import tpu as pltpu
from jax.sharding import PartitionSpec as P

BF = jnp.bfloat16
F32 = jnp.float32
BC = 256
NB = 12
NX = 4


def dot(a, b):
    return jnp.dot(a, b, preferred_element_type=F32)


def kernel(
    n, el, cap, x_ref, meta_ref, wg_ref, wu_ref, wd_ref,
    y_ref, rl_ref,
    acc_g, acc_u, dmat, wmat, xbuf, zbuf, wbuf, ybuf, meta,
    wsem, xsem, xs_send, xs_recv, m_send, m_recv, o_send, o_recv, l_send, l_recv, st_sem, y_sem, credit,
):
    tokens, d = x_ref.shape
    ff = wg_ref.shape[2]
    nc = d // BC
    half = tokens // 2
    rows = n * cap
    per = el * cap
    me = lax.axis_index("ep")
    right, left, opp = lax.rem(me + 1, n), lax.rem(me + n - 1, n), lax.rem(me + 2, n)
    tiles1 = nc * el * 2


    def start_gu(c, e):
        for i, w in enumerate((wg_ref, wu_ref)):
            s = lax.rem(c * (2 * el) + 2 * e + i, NB)
            pltpu.make_async_copy(w.at[e, pl.ds(c * BC, BC)], wbuf.at[s], wsem.at[s]).start()

    def start_dn(c, e):
        s = lax.rem(tiles1 + c * el + e, NB)
        for j in range(ff // BC):
            pltpu.make_async_copy(
                wd_ref.at[e, pl.ds(j * BC, BC), pl.ds(c * BC, BC)], wbuf.at[s, :, pl.ds(j * BC, BC)], wsem.at[s]
            ).start()

    def wait_tile(q):
        s = lax.rem(q, NB)
        pltpu.make_async_copy(wbuf.at[s], wbuf.at[s], wsem.at[s]).wait()
        return s

    for e in range(NB // 2):
        start_gu(0, e)

    def load_own(c):
        return pltpu.make_async_copy(x_ref.at[:, pl.ds(c * BC, BC)], xbuf.at[lax.rem(c, NX), 0], xsem.at[lax.rem(c, NX)])


    for c in range(NX):
        load_own(c).start()

    def send(src, dst, ss, rs, to):
        return pltpu.make_async_remote_copy(
            src_ref=src, dst_ref=dst, send_sem=ss, recv_sem=rs, device_id={"ep": to},
            device_id_type=pl.DeviceIdType.MESH,
        )

    def own(c, direction, part):
        h = part if direction == 0 else 1 - part
        i = 2 * direction + part
        return send(
            xbuf.at[lax.rem(c, NX), 0, pl.ds(h * half, half)],
            xbuf.at[lax.rem(c, NX), 1 + direction, pl.ds(h * half, half)],
            xs_send.at[i, c], xs_recv.at[i, c], (right, left)[direction],
        )

    def forward(c, direction):
        h = direction
        return send(
            xbuf.at[lax.rem(c, NX), 1 + direction, pl.ds(h * half, half)],
            xbuf.at[lax.rem(c, NX), 3, pl.ds(h * half, half)],
            xs_send.at[4 + direction, c], xs_recv.at[4 + direction, c], (right, left)[direction],
        )

    def both(c, part):
        for direction in range(2):
            own(c, direction, part).start()

    def service(c, again):
        @pl.when(c < nc)
        def _():
            for direction in range(2):
                own(c, direction, 0).wait_recv()
                forward(c, direction).start()

        @pl.when(c + 1 < nc)
        def _():
            both(c + 1, 1)

        @pl.when(c + 2 < nc)
        def _():
            if again:
                load_own(c + 2).wait()
                for direction in range(2):
                    pl.semaphore_wait(credit.at[direction], 1)
            both(c + 2, 0)

    barrier = pltpu.get_barrier_semaphore()
    for to in (left, right, opp):
        pl.semaphore_signal(barrier, inc=1, device_id={"ep": to}, device_id_type=pl.DeviceIdType.MESH)
    pl.semaphore_wait(barrier, 3)

    metas = [
        send(meta_ref, meta.at[1 + i], m_send.at[i], m_recv.at[i], to) for i, to in enumerate((right, left, opp))
    ]
    for m in metas:
        m.start()
    load_own(0).wait()
    both(0, 0)
    both(0, 1)
    meta[0] = meta_ref[...]

    top = meta_ref.shape[0] // 2
    base = (me * per).astype(F32)
    first = lax.broadcasted_iota(jnp.int32, (el, tokens), 0).astype(F32) * cap + base
    line = lax.broadcasted_iota(jnp.int32, (cap, tokens), 0).astype(F32)

    def build(b, _):
        @pl.when(b == 1)
        def _():
            for m in metas:
                m.wait_recv()

        s = jnp.full((el, tokens), -1.0, F32)
        g = jnp.zeros((el, tokens), F32)
        for k in range(top):
            r = meta[b, pl.ds(k, 1)] - first
            ok = jnp.logical_and(r >= 0.0, r < cap)
            s = jnp.where(ok, r, s)
            g = jnp.where(ok, meta[b, pl.ds(top + k, 1)], g)
        acc_u[0, pl.ds(0, el), pl.ds(0, tokens)] = s
        acc_u[1, pl.ds(0, el), pl.ds(0, tokens)] = g

        def lines(e, _):
            eq = acc_u[0, pl.ds(e, 1), pl.ds(0, tokens)] == line
            at = pl.multiple_of(e * cap, 16)
            dmat[b, pl.ds(at, cap)] = jnp.where(eq, 1.0, 0.0).astype(BF)
            w = jnp.where(eq, acc_u[1, pl.ds(e, 1), pl.ds(0, tokens)], 0.0).astype(BF)
            for j in range(tokens // BC):
                zbuf[pl.ds(pl.multiple_of(j * per + e * cap, 16), cap)] = w[:, j * BC : (j + 1) * BC]
            return 0

        lax.fori_loop(0, el, lines, 0)
        for i in range(per // 128):
            for j in range(tokens // BC):
                t = zbuf[pl.ds(j * per + i * 128, 128)]
                wmat[b, pl.ds(j * BC, BC), pl.ds(i * 128, 128)] = t.T

        @pl.when(b == 0)
        def _():
            for direction in range(2):
                own(0, direction, 0).wait_recv()
                forward(0, direction).start()
            for c in range(1, NX):
                load_own(c).wait()
            both(1, 0)
            both(1, 1)
            both(2, 0)

        return 0

    lax.fori_loop(0, n, build, 0)

    def gate_up(c, p, first, last):
        q = c * (2 * el) + 4 * p
        slots = [wait_tile(q + i) for i in range(4)]
        for u in range(2):
            e = 2 * p + u
            z = zbuf[pl.ds(pl.multiple_of(e * rows, 16), rows)]
            for j in range(ff // BC):
                cols = pl.ds(j * BC, BC)
                g = dot(z, wbuf[slots[2 * u], :, cols])
                v = dot(z, wbuf[slots[2 * u + 1], :, cols])
                if not first:
                    g = acc_g[e, :, cols] + g
                    v = acc_u[e, :, cols] + v
                if last:
                    acc_g[e, :, cols] = (g * jax.nn.sigmoid(g) * v).astype(BF).astype(F32)
                else:
                    acc_g[e, :, cols] = g
                    acc_u[e, :, cols] = v
        ahead = 2 * p + NB // 2
        if last:

            @pl.when(ahead < el)
            def _():
                for u in range(2):
                    start_gu(c, ahead + u)

            @pl.when(ahead >= el)
            def _():
                for u in range(4):
                    start_dn(0, 2 * (ahead - el) + u)
        else:
            over = (ahead >= el).astype(jnp.int32)
            for u in range(2):
                start_gu(c + over, ahead + u - over * el)

    def phase1(c, first=False, last=False):
        slot = lax.rem(c, NX)
        if not (first or last):
            service(c + 1, True)
        for direction in range(2):
            own(c, direction, 1).wait_recv()
        for direction in range(2):
            forward(c, direction).wait_recv()
        for b in range(n):
            z = dot(dmat[b], xbuf[slot, b]).astype(BF)
            for e in range(el):
                zbuf[pl.ds(e * rows + b * cap, cap)] = z[e * cap : (e + 1) * cap]
        for direction in range(2):
            own(c, direction, 0).wait_send()
            own(c, direction, 1).wait_send()
            forward(c, direction).wait_send()

        def free():
            for direction, to in enumerate((left, right)):
                pl.semaphore_signal(
                    credit.at[direction], inc=1, device_id={"ep": to}, device_id_type=pl.DeviceIdType.MESH
                )

        if last:
            free()
        else:
            pl.when(c + NX < nc)(free)
        def body(p, _):
            gate_up(c, p, first, last)
            return 0

        lax.fori_loop(0, el // 4, body, 0)
        if first:
            service(c + 1, False)
        if not last:

            @pl.when(c + NX < nc)
            def _():
                load_own(c + NX).start()

        lax.fori_loop(el // 4, el // 2, body, 0)

    def loop1(c, _):
        phase1(c)
        return 0

    phase1(0, first=True)
    lax.fori_loop(1, nc - 1, loop1, 0)
    phase1(nc - 1, last=True)

    def keep(kind, c, i, value):
        acc_u[2 * c + i, pl.ds(0, half), pl.ds(kind * BC, BC)] = value

    def kept(kind, c, i):
        return acc_u[2 * c + i, pl.ds(0, half), pl.ds(kind * BC, BC)]

    def sl_at(slot, i):
        block = 2 + 2 * slot + i
        return xbuf.at[block // n, lax.rem(block, n)]

    def ro_at(c, i):
        return xbuf.at[2 + c // n, lax.rem(c, n), pl.ds(i * half, half)]

    def put_o(slot, r, value):
        xbuf[0, slot, r] = value

    def send_o(c, i):
        slot = lax.rem(c, 2)
        return send(
            xbuf.at[0, slot, pl.ds(i * half, half)], ro_at(c, i), o_send.at[i, slot], o_recv.at[i, c],
            (left, right)[i],
        )

    def send_l(c, i):
        slot = lax.rem(c, 2)
        return send(
            sl_at(slot, i), rl_ref.at[c, i], l_send.at[i, slot], l_recv.at[i, c], (left, right)[i]
        )

    def stage_l(c):
        return pltpu.make_async_copy(rl_ref.at[c], xbuf.at[1, pl.ds(2, 2)], st_sem.at[1])

    def out_y(c):
        return pltpu.make_async_copy(ybuf, y_ref.at[:, pl.ds(c * BC, BC)], y_sem.at[0])

    def arrive_o(c):
        for i in range(2):
            send_o(c, i).wait_recv()

    def arrive_l(c):
        for i in range(2):
            send_l(c, i).wait_recv()
        stage_l(c).start()

    def pass_on(c):
        slot = lax.rem(c, 2)

        @pl.when(c >= 2)
        def _():
            for i in range(2):
                send_l(c - 2, i).wait_send()

        for i in range(2):
            to = sl_at(slot, i)
            to[pl.ds(i * half, half)] = (kept(1 + i, c, i) + ro_at(c, i)[...].astype(F32)).astype(BF)
            to[pl.ds((1 - i) * half, half)] = kept(1 + i, c, 1 - i).astype(BF)
            send_l(c, i).start()

    def finish(c):
        stage_l(c).wait()

        @pl.when(c >= 1)
        def _():
            out_y(c - 1).wait()

        for i in range(2):
            r = pl.ds(i * half, half)
            ybuf[r] = (kept(0, c, i) + xbuf[1, 2, r].astype(F32) + xbuf[1, 3, r].astype(F32)).astype(BF)
        out_y(c).start()

    def phase2(c, _):
        def down(p, _):
            q = tiles1 + c * el + 4 * p
            slots = [wait_tile(q + i) for i in range(4)]
            for u in range(4):
                e = 4 * p + u
                w = jnp.concatenate([wbuf[slots[u], :, pl.ds(j * BC, BC)] for j in range(ff // BC)], axis=0)
                o = dot(acc_g[e].astype(BF), w).astype(BF)
                for b in range(n):
                    zbuf[pl.ds(pl.multiple_of(b * per + e * cap, 16), cap)] = o[b * cap : (b + 1) * cap]
            r = c * el + 4 * p + NB

            @pl.when(r < nc * el)
            def _():
                for i in range(4):
                    start_dn(r // el, lax.rem(r, el) + i)

            return 0

        lax.fori_loop(0, el // 4, down, 0)

        slot = lax.rem(c, 2)

        @pl.when(c >= 2)
        def _():
            for i in range(2):
                send_o(c - 2, i).wait_send()

        for i in range(2):
            r = pl.ds(i * half, half)
            put_o(slot, r, dot(wmat[3, r], zbuf[pl.ds(3 * per, per)]).astype(BF))
        @pl.when(c == 0)
        def _():
            for i in range(2):
                pl.semaphore_wait(credit.at[i], 1)

        for i in range(2):
            send_o(c, i).start()

        @pl.when(c >= 1)
        def _():
            arrive_o(c - 1)

        @pl.when(c >= 3)
        def _():
            arrive_l(c - 3)

        for kind in range(3):
            for i in range(2):
                keep(kind, c, i, dot(wmat[kind, pl.ds(i * half, half)], zbuf[pl.ds(kind * per, per)]))

        @pl.when(c >= 1)
        def _():
            pass_on(c - 1)

        @pl.when(c >= 3)
        def _():
            finish(c - 3)

        return 0

    lax.fori_loop(0, nc, phase2, 0)
    arrive_o(nc - 1)
    pass_on(nc - 1)
    for c in (nc - 3, nc - 2, nc - 1):
        arrive_l(c)
        finish(c)
    out_y(nc - 1).wait()
    for c in (nc - 2, nc - 1):
        for i in range(2):
            send_o(c, i).wait_send()
            send_l(c, i).wait_send()

    for m in metas:
        m.wait_send()


def solution(mesh):
    n = mesh.shape["ep"]

    def step(x, expert, slot, gate, w_gate, w_up, w_down):
        x, expert, slot, gate = (v[0, 0] for v in (x, expert, slot, gate))
        tokens, d = x.shape
        el, _, ff = w_gate.shape
        top = expert.shape[1]
        cap = 5 * tokens * top // (4 * el * n)
        nc = d // BC
        half = tokens // 2
        key = jnp.where(slot < cap, expert * cap + slot, -1)
        meta = jnp.concatenate([key.astype(F32).T, gate.astype(BF).astype(F32).T], 0)
        any_, vmem = pl.BlockSpec(memory_space=pl.ANY), pl.BlockSpec(memory_space=pltpu.VMEM)
        dma = pltpu.SemaphoreType.DMA
        y, *_ = pl.pallas_call(
            functools.partial(kernel, n, el, cap),
            out_shape=[
                jax.ShapeDtypeStruct((tokens, d), BF),
                jax.ShapeDtypeStruct((nc, 2, tokens, BC), BF),
            ],
            in_specs=[any_, vmem, any_, any_, any_],
            out_specs=[any_] * 2,
            scratch_shapes=[
                pltpu.VMEM((el, n * cap, ff), F32),
                pltpu.VMEM((el, n * cap, ff), F32),
                pltpu.VMEM((n, el * cap, tokens), BF),
                pltpu.VMEM((n, tokens, el * cap), BF),
                pltpu.VMEM((NX, n, tokens, BC), BF),
                pltpu.VMEM((n * el * cap, BC), BF),
                pltpu.VMEM((NB, BC, ff), BF),
                pltpu.VMEM((tokens, BC), BF),
                pltpu.VMEM((n, 2 * top, tokens), F32),
                dma((NB,)),
                dma((NX,)),
                dma((6, nc)),
                dma((6, nc)),
                dma((3,)),
                dma((3,)),
                dma((2, 2)),
                dma((2, nc)),
                dma((2, 2)),
                dma((2, nc)),
                dma((2,)),
                dma((1,)),
                pltpu.SemaphoreType.REGULAR((2,)),
            ],
            compiler_params=pltpu.CompilerParams(
                collective_id=0, has_side_effects=True, vmem_limit_bytes=67043328
            ),
        )(x, meta, w_gate, w_up, w_down)
        return y[None, None]

    token, weight = P("dp", "ep", None, None), P("ep", None, None)
    return jax.shard_map(
        step,
        mesh=mesh,
        in_specs=(token,) * 4 + (weight,) * 3,
        out_specs=token,
        check_vma=False,
    )
```

```python
import functools

import jax
import jax.numpy as jnp
from jax import lax
from jax.experimental import pallas as pl
from jax.experimental.pallas import tpu as pltpu
from jax.sharding import PartitionSpec as P

BF = jnp.bfloat16
F32 = jnp.float32
BC = 256
NB = 12
NX = 4
PIECES = 4


def dot(a, b):
    return jnp.dot(a, b, preferred_element_type=F32)


def kernel(
    n, el, cap, x_ref, expert_ref, slot_ref, gate_ref, wg_ref, wu_ref, wd_ref,
    y_ref, rl_ref, last_ref, own_ref,
    acc_g, acc_u, dmat, wmat, xbuf, zbuf, wbuf, ybuf, meta,
    wsem, xsem, xs_send, xs_recv, m_send, m_recv, o_send, o_recv, l_send, l_recv, st_sem, y_sem, own_sem, credit,
):
    tokens, d = x_ref.shape
    ff = wg_ref.shape[2]
    nc = d // BC
    half = tokens // 2
    rows = n * cap
    per = el * cap
    me = lax.axis_index("ep")
    right, left, opp = lax.rem(me + 1, n), lax.rem(me + n - 1, n), lax.rem(me + 2, n)
    tiles1 = nc * el * 2


    def start_gu(c, e):
        for i, w in enumerate((wg_ref, wu_ref)):
            s = lax.rem(c * (2 * el) + 2 * e + i, NB)
            pltpu.make_async_copy(w.at[e, pl.ds(c * BC, BC)], wbuf.at[s], wsem.at[s]).start()

    def start_dn(c, e):
        s = lax.rem(tiles1 + c * el + e, NB)
        for j in range(ff // BC):
            pltpu.make_async_copy(
                wd_ref.at[e, pl.ds(j * BC, BC), pl.ds(c * BC, BC)], wbuf.at[s, :, pl.ds(j * BC, BC)], wsem.at[s]
            ).start()

    def wait_tile(q):
        s = lax.rem(q, NB)
        pltpu.make_async_copy(wbuf.at[s], wbuf.at[s], wsem.at[s]).wait()
        return s

    def load_own(c):
        return pltpu.make_async_copy(x_ref.at[:, pl.ds(c * BC, BC)], xbuf.at[lax.rem(c, NX), 0], xsem.at[lax.rem(c, NX)])


    load_own(0).start()

    def send(src, dst, ss, rs, to):
        return pltpu.make_async_remote_copy(
            src_ref=src, dst_ref=dst, send_sem=ss, recv_sem=rs, device_id={"ep": to},
            device_id_type=pl.DeviceIdType.MESH,
        )

    def own(c, direction, part):
        h = part if direction == 0 else 1 - part
        i = 2 * direction + part
        return send(
            xbuf.at[lax.rem(c, NX), 0, pl.ds(h * half, half)],
            xbuf.at[lax.rem(c, NX), 1 + direction, pl.ds(h * half, half)],
            xs_send.at[i, c], xs_recv.at[i, c], (right, left)[direction],
        )

    def forward(c, direction):
        h = direction
        return send(
            xbuf.at[lax.rem(c, NX), 1 + direction, pl.ds(h * half, half)],
            xbuf.at[lax.rem(c, NX), 3, pl.ds(h * half, half)],
            xs_send.at[4 + direction, c], xs_recv.at[4 + direction, c], (right, left)[direction],
        )

    def both(c, part):
        for direction in range(2):
            own(c, direction, part).start()

    def service(c, again):
        @pl.when(c < nc)
        def _():
            for direction in range(2):
                own(c, direction, 0).wait_recv()
                forward(c, direction).start()

        @pl.when(c + 1 < nc)
        def _():
            both(c + 1, 1)

        @pl.when(c + 2 < nc)
        def _():
            if again:
                load_own(c + 2).wait()
                for direction in range(2):
                    pl.semaphore_wait(credit.at[direction], 1)
            both(c + 2, 0)

    top = expert_ref.shape[0]
    slot = slot_ref[...]
    meta[0, pl.ds(0, top)] = jnp.where(slot < cap, expert_ref[...] * cap + slot, -1).astype(F32)
    meta[0, pl.ds(top, top)] = gate_ref[...]

    barrier = pltpu.get_barrier_semaphore()
    for to in (left, right, opp):
        pl.semaphore_signal(barrier, inc=1, device_id={"ep": to}, device_id_type=pl.DeviceIdType.MESH)
    pl.semaphore_wait(barrier, 3)

    metas = [
        send(meta.at[0], meta.at[1 + i], m_send.at[i], m_recv.at[i], to) for i, to in enumerate((right, left, opp))
    ]
    load_own(0).wait()
    both(0, 0)
    for m in metas:
        m.start()
    both(0, 1)
    for c in range(1, NX):
        load_own(c).start()
    for e in range(NB // 2):
        start_gu(0, e)
    base = (me * per).astype(F32)
    first = lax.broadcasted_iota(jnp.int32, (el, tokens), 0).astype(F32) * cap + base
    line = lax.broadcasted_iota(jnp.int32, (cap, tokens), 0).astype(F32)

    def build(b, _):
        @pl.when(b == 1)
        def _():
            for m in metas:
                m.wait_recv()

        s = jnp.full((el, tokens), -1.0, F32)
        g = jnp.zeros((el, tokens), F32)
        for k in range(top):
            r = meta[b, pl.ds(k, 1)] - first
            ok = jnp.logical_and(r >= 0.0, r < cap)
            s = jnp.where(ok, r, s)
            g = jnp.where(ok, meta[b, pl.ds(top + k, 1)], g)
        acc_u[0, pl.ds(0, el), pl.ds(0, tokens)] = s
        acc_u[1, pl.ds(0, el), pl.ds(0, tokens)] = g

        def lines(e, _):
            eq = acc_u[0, pl.ds(e, 1), pl.ds(0, tokens)] == line
            at = pl.multiple_of(e * cap, 16)
            dmat[b, pl.ds(at, cap)] = jnp.where(eq, 1.0, 0.0).astype(BF)
            w = jnp.where(eq, acc_u[1, pl.ds(e, 1), pl.ds(0, tokens)], 0.0).astype(BF)
            for j in range(tokens // BC):
                zbuf[pl.ds(pl.multiple_of(j * per + e * cap, 16), cap)] = w[:, j * BC : (j + 1) * BC]
            return 0

        lax.fori_loop(0, el, lines, 0, unroll=2)
        for i in range(per // 128):
            for j in range(tokens // BC):
                t = zbuf[pl.ds(j * per + i * 128, 128)]
                wmat[b, pl.ds(j * BC, BC), pl.ds(i * 128, 128)] = t.T

        @pl.when(b == 0)
        def _():
            for direction in range(2):
                own(0, direction, 0).wait_recv()
                forward(0, direction).start()
            for c in range(1, NX):
                load_own(c).wait()
            both(1, 0)
            both(1, 1)
            both(2, 0)

        return 0

    lax.fori_loop(0, n, build, 0)

    def gate_up(c, p, first, last):
        q = c * (2 * el) + 4 * p
        slots = [wait_tile(q + i) for i in range(4)]
        for u in range(2):
            e = 2 * p + u
            z = zbuf[pl.ds(pl.multiple_of(e * rows, 16), rows)]
            for j in range(ff // BC):
                cols = pl.ds(j * BC, BC)
                g = dot(z, wbuf[slots[2 * u], :, cols])
                v = dot(z, wbuf[slots[2 * u + 1], :, cols])
                if not first:
                    g = acc_g[e, :, cols] + g
                    v = acc_u[e, :, cols] + v
                if last:
                    acc_g[e, :, cols] = (g * jax.nn.sigmoid(g) * v).astype(BF).astype(F32)
                else:
                    acc_g[e, :, cols] = g
                    acc_u[e, :, cols] = v
        ahead = 2 * p + NB // 2
        if last:

            @pl.when(ahead < el)
            def _():
                for u in range(2):
                    start_gu(c, ahead + u)

            @pl.when(ahead >= el)
            def _():
                for u in range(4):
                    start_dn(0, 2 * (ahead - el) + u)
        else:
            over = (ahead >= el).astype(jnp.int32)
            for u in range(2):
                start_gu(c + over, ahead + u - over * el)

    def phase1(c, first=False, last=False):
        slot = lax.rem(c, NX)
        if not (first or last):
            service(c + 1, True)
        for direction in range(2):
            own(c, direction, 1).wait_recv()
        for b in range(n):
            if b == 3:
                for direction in range(2):
                    forward(c, direction).wait_recv()
            for i in range(2):
                z = dot(dmat[b, pl.ds(i * (per // 2), per // 2)], xbuf[slot, b]).astype(BF)
                for e in range(el // 2):
                    zbuf[pl.ds((i * (el // 2) + e) * rows + b * cap, cap)] = z[e * cap : (e + 1) * cap]
        for direction in range(2):
            own(c, direction, 0).wait_send()
            own(c, direction, 1).wait_send()
            forward(c, direction).wait_send()

        def free():
            for direction, to in enumerate((left, right)):
                pl.semaphore_signal(
                    credit.at[direction], inc=1, device_id={"ep": to}, device_id_type=pl.DeviceIdType.MESH
                )

        if last:
            free()
        else:
            pl.when(c + NX < nc)(free)
        def body(p, _):
            gate_up(c, p, first, last)
            return 0

        if first:
            service(c + 1, False)
        lax.fori_loop(0, el // 4, body, 0)
        if not last:

            @pl.when(c + NX < nc)
            def _():
                load_own(c + NX).start()

        lax.fori_loop(el // 4, el // 2, body, 0)

    def loop1(c, _):
        phase1(c)
        return 0

    phase1(0, first=True)
    lax.fori_loop(1, nc - 1, loop1, 0)
    phase1(nc - 1, last=True)

    def keep(kind, c, i, value):
        acc_u[2 * c + i, pl.ds(0, half), pl.ds(kind * BC, BC)] = value

    def kept(kind, c, i):
        return acc_u[2 * c + i, pl.ds(0, half), pl.ds(kind * BC, BC)]

    def sl_at(slot, i):
        block = 2 + 2 * slot + i
        return xbuf.at[block // n, lax.rem(block, n)]

    def ro_at(c, i):
        return xbuf.at[2 + c // n, lax.rem(c, n), pl.ds(i * half, half)]

    def put_o(slot, r, value):
        xbuf[0, slot, r] = value

    def send_o(c, i):
        slot = lax.rem(c, 2)
        return send(
            xbuf.at[0, slot, pl.ds(i * half, half)], ro_at(c, i), o_send.at[i, slot], o_recv.at[i, c],
            (left, right)[i],
        )

    def send_l(c, i):
        slot = lax.rem(c, 2)
        return send(
            sl_at(slot, i), last_ref.at[i] if isinstance(c, int) and c == nc - 1 else rl_ref.at[c, i], l_send.at[i, slot], l_recv.at[i, c], (left, right)[i]
        )

    def stage_l(c):
        return pltpu.make_async_copy(rl_ref.at[c], xbuf.at[1, pl.ds(2, 2)], st_sem.at[1])

    def out_y(c):
        return pltpu.make_async_copy(ybuf, y_ref.at[:, pl.ds(c * BC, BC)], y_sem.at[0])

    def out_own(i):
        return pltpu.make_async_copy(
            acc_u.at[2 * (nc - 1) + i, pl.ds(0, half), pl.ds(0, BC)], own_ref.at[pl.ds(i * half, half)], own_sem.at[i]
        )

    def arrive_o(c):
        for i in range(2):
            send_o(c, i).wait_recv()

    def arrive_l(c):
        for i in range(2):
            send_l(c, i).wait_recv()
        stage_l(c).start()

    def pass_on(c):
        slot = lax.rem(c, 2)

        @pl.when(c >= 2)
        def _():
            for i in range(2):
                send_l(c - 2, i).wait_send()

        for i in range(2):
            to = sl_at(slot, i)
            to[pl.ds(i * half, half)] = (kept(1 + i, c, i) + ro_at(c, i)[...].astype(F32)).astype(BF)
            to[pl.ds((1 - i) * half, half)] = kept(1 + i, c, 1 - i).astype(BF)
            send_l(c, i).start()

    def finish(c):
        stage_l(c).wait()

        @pl.when(c >= 1)
        def _():
            out_y(c - 1).wait()

        for i in range(2):
            r = pl.ds(i * half, half)
            ybuf[r] = (kept(0, c, i) + xbuf[1, 2, r].astype(F32) + xbuf[1, 3, r].astype(F32)).astype(BF)
        out_y(c).start()

    def phase2(c, _):
        def down(p, _):
            q = tiles1 + c * el + 4 * p
            slots = [wait_tile(q + i) for i in range(4)]
            for u in range(4):
                e = 4 * p + u
                w = jnp.concatenate([wbuf[slots[u], :, pl.ds(j * BC, BC)] for j in range(ff // BC)], axis=0)
                o = dot(acc_g[e].astype(BF), w).astype(BF)
                for b in range(n):
                    zbuf[pl.ds(pl.multiple_of(b * per + e * cap, 16), cap)] = o[b * cap : (b + 1) * cap]
            r = c * el + 4 * p + NB

            @pl.when(r < nc * el)
            def _():
                for i in range(4):
                    start_dn(r // el, lax.rem(r, el) + i)

            return 0

        lax.fori_loop(0, el // 4, down, 0)

        slot = lax.rem(c, 2)

        @pl.when(c >= 2)
        def _():
            for i in range(2):
                send_o(c - 2, i).wait_send()

        for i in range(2):
            r = pl.ds(i * half, half)
            put_o(slot, r, dot(wmat[3, r], zbuf[pl.ds(3 * per, per)]).astype(BF))
        @pl.when(c == 0)
        def _():
            for i in range(2):
                pl.semaphore_wait(credit.at[i], 1)

        for i in range(2):
            send_o(c, i).start()

        @pl.when(c >= 1)
        def _():
            arrive_o(c - 1)

        @pl.when(c >= 3)
        def _():
            arrive_l(c - 3)

        for kind in range(3):
            for i in range(2):
                keep(kind, c, i, dot(wmat[kind, pl.ds(i * half, half)], zbuf[pl.ds(kind * per, per)]))

        @pl.when(c >= 1)
        def _():
            pass_on(c - 1)

        @pl.when(c >= 3)
        def _():
            finish(c - 3)

        return 0

    lax.fori_loop(0, nc, phase2, 0)
    for i in range(2):
        out_own(i).start()
    arrive_o(nc - 1)
    pass_on(nc - 1)
    for c in (nc - 3, nc - 2):
        arrive_l(c)
        finish(c)
    out_y(nc - 2).wait()
    for i in range(2):
        out_own(i).wait()
        send_l(nc - 1, i).wait_recv()
    for c in (nc - 2, nc - 1):
        for i in range(2):
            send_o(c, i).wait_send()
            send_l(c, i).wait_send()

    for m in metas:
        m.wait_send()


def end_kernel(most_ref, last_ref, own_ref, y_ref, most, last, own, end, in_sem, out_sem, sem):
    tokens, width = most.shape
    lasts = [
        pltpu.make_async_copy(last_ref, last, sem.at[0]),
        pltpu.make_async_copy(own_ref, own, sem.at[1]),
    ]
    rows = [pl.ds(i * (tokens // PIECES), tokens // PIECES) for i in range(PIECES)]
    ins = [pltpu.make_async_copy(most_ref.at[r], most.at[r], in_sem.at[i]) for i, r in enumerate(rows)]
    outs = [pltpu.make_async_copy(most.at[r], y_ref.at[r, pl.ds(0, width)], out_sem.at[i]) for i, r in enumerate(rows)]
    for c in lasts + ins:
        c.start()
    for c in lasts:
        c.wait()
    end[...] = (own[...] + last[0].astype(F32) + last[1].astype(F32)).astype(BF)
    final = pltpu.make_async_copy(end, y_ref.at[:, pl.ds(width, end.shape[1])], sem.at[2])
    final.start()
    for i, o in zip(ins, outs):
        i.wait()
        o.start()
    for o in outs:
        o.wait()
    final.wait()


def solution(mesh):
    n = mesh.shape["ep"]

    def step(x, expert, slot, gate, w_gate, w_up, w_down):
        x, expert, slot, gate = (v[0, 0] for v in (x, expert, slot, gate))
        tokens, d = x.shape
        el, _, ff = w_gate.shape
        top = expert.shape[1]
        cap = 5 * tokens * top // (4 * el * n)
        nc = d // BC
        any_, vmem = pl.BlockSpec(memory_space=pl.ANY), pl.BlockSpec(memory_space=pltpu.VMEM)
        dma = pltpu.SemaphoreType.DMA
        y, _, last, own = pl.pallas_call(
            functools.partial(kernel, n, el, cap),
            out_shape=[
                jax.ShapeDtypeStruct((tokens, d - BC), BF),
                jax.ShapeDtypeStruct((nc - 1, 2, tokens, BC), BF),
                jax.ShapeDtypeStruct((2, tokens, BC), BF),
                jax.ShapeDtypeStruct((tokens, BC), F32),
            ],
            in_specs=[any_, vmem, vmem, vmem, any_, any_, any_],
            out_specs=[any_] * 4,
            scratch_shapes=[
                pltpu.VMEM((el, n * cap, ff), F32),
                pltpu.VMEM((el, n * cap, ff), F32),
                pltpu.VMEM((n, el * cap, tokens), BF),
                pltpu.VMEM((n, tokens, el * cap), BF),
                pltpu.VMEM((NX, n, tokens, BC), BF),
                pltpu.VMEM((n * el * cap, BC), BF),
                pltpu.VMEM((NB, BC, ff), BF),
                pltpu.VMEM((tokens, BC), BF),
                pltpu.VMEM((n, 2 * top, tokens), F32),
                dma((NB,)),
                dma((NX,)),
                dma((6, nc)),
                dma((6, nc)),
                dma((3,)),
                dma((3,)),
                dma((2, 2)),
                dma((2, nc)),
                dma((2, 2)),
                dma((2, nc)),
                dma((2,)),
                dma((1,)),
                dma((2,)),
                pltpu.SemaphoreType.REGULAR((2,)),
            ],
            compiler_params=pltpu.CompilerParams(
                collective_id=0, has_side_effects=True, vmem_limit_bytes=67043328
            ),
        )(x, expert.T, slot.T, gate.T, w_gate, w_up, w_down)
        y = pl.pallas_call(
            end_kernel,
            out_shape=jax.ShapeDtypeStruct((tokens, d), BF),
            in_specs=[any_] * 3,
            out_specs=any_,
            scratch_shapes=[
                pltpu.VMEM((tokens, d - BC), BF),
                pltpu.VMEM((2, tokens, BC), BF),
                pltpu.VMEM((tokens, BC), F32),
                pltpu.VMEM((tokens, BC), BF),
                dma((PIECES,)),
                dma((PIECES,)),
                dma((3,)),
            ],
            compiler_params=pltpu.CompilerParams(vmem_limit_bytes=67043328),
        )(y, last, own)
        return y[None, None]

    token, weight = P("dp", "ep", None, None), P("ep", None, None)
    return jax.shard_map(
        step,
        mesh=mesh,
        in_specs=(token,) * 4 + (weight,) * 3,
        out_specs=token,
        check_vma=False,
    )
```

```python
import functools

import jax
import jax.numpy as jnp
from jax import lax
from jax.experimental import pallas as pl
from jax.experimental.pallas import tpu as pltpu
from jax.sharding import PartitionSpec as P

BF = jnp.bfloat16
F32 = jnp.float32
BC = 256
NB = 12
NX = 4
PIECES = 4


def dot(a, b):
    return jnp.dot(a, b, preferred_element_type=F32)


def kernel(
    n, el, cap, x_ref, expert_ref, slot_ref, gate_ref, wg_ref, wu_ref, wd_ref,
    y_ref, rl_ref, last_ref, own_ref,
    acc_g, acc_u, dmat, wmat, xbuf, zbuf, wbuf, ybuf, meta,
    wsem, xsem, xs_send, xs_recv, m_send, m_recv, o_send, o_recv, l_send, l_recv, st_sem, y_sem, own_sem, credit,
):
    tokens, d = x_ref.shape
    ff = wg_ref.shape[2]
    nc = d // BC
    half = tokens // 2
    rows = n * cap
    per = el * cap
    me = lax.axis_index("ep")
    right, left, opp = lax.rem(me + 1, n), lax.rem(me + n - 1, n), lax.rem(me + 2, n)
    tiles1 = nc * el * 2


    def start_gu(c, e):
        for i, w in enumerate((wg_ref, wu_ref)):
            s = lax.rem(c * (2 * el) + 2 * e + i, NB)
            for j in range(2):
                pltpu.make_async_copy(
                    w.at[e, pl.ds(c * BC + j * (BC // 2), BC // 2)], wbuf.at[s, pl.ds(j * (BC // 2), BC // 2)], wsem.at[s]
                ).start()

    def start_dn(c, e):
        s = lax.rem(tiles1 + c * el + e, NB)
        for j in range(ff // BC):
            pltpu.make_async_copy(
                wd_ref.at[e, pl.ds(j * BC, BC), pl.ds(c * BC, BC)], wbuf.at[s, :, pl.ds(j * BC, BC)], wsem.at[s]
            ).start()

    def wait_tile(q):
        s = lax.rem(q, NB)
        pltpu.make_async_copy(wbuf.at[s], wbuf.at[s], wsem.at[s]).wait()
        return s

    def load_own(c):
        return pltpu.make_async_copy(x_ref.at[:, pl.ds(c * BC, BC)], xbuf.at[lax.rem(c, NX), 0], xsem.at[lax.rem(c, NX)])


    load_own(0).start()

    def send(src, dst, ss, rs, to):
        return pltpu.make_async_remote_copy(
            src_ref=src, dst_ref=dst, send_sem=ss, recv_sem=rs, device_id={"ep": to},
            device_id_type=pl.DeviceIdType.MESH,
        )

    def own(c, direction, part):
        h = part if direction == 0 else 1 - part
        i = 2 * direction + part
        return send(
            xbuf.at[lax.rem(c, NX), 0, pl.ds(h * half, half)],
            xbuf.at[lax.rem(c, NX), 1 + direction, pl.ds(h * half, half)],
            xs_send.at[i, c], xs_recv.at[i, c], (right, left)[direction],
        )

    def forward(c, direction):
        h = direction
        return send(
            xbuf.at[lax.rem(c, NX), 1 + direction, pl.ds(h * half, half)],
            xbuf.at[lax.rem(c, NX), 3, pl.ds(h * half, half)],
            xs_send.at[4 + direction, c], xs_recv.at[4 + direction, c], (right, left)[direction],
        )

    def both(c, part):
        for direction in range(2):
            own(c, direction, part).start()

    def service(c, again):
        @pl.when(c < nc)
        def _():
            for direction in range(2):
                own(c, direction, 0).wait_recv()
                forward(c, direction).start()

        @pl.when(c + 1 < nc)
        def _():
            both(c + 1, 1)

        @pl.when(c + 2 < nc)
        def _():
            if again:
                load_own(c + 2).wait()
                for direction in range(2):
                    pl.semaphore_wait(credit.at[direction], 1)
            both(c + 2, 0)

    top = expert_ref.shape[0]
    slot = slot_ref[...]
    meta[0, pl.ds(0, top)] = jnp.where(slot < cap, expert_ref[...] * cap + slot, -1).astype(F32)
    meta[0, pl.ds(top, top)] = gate_ref[...]

    barrier = pltpu.get_barrier_semaphore()
    for to in (left, right, opp):
        pl.semaphore_signal(barrier, inc=1, device_id={"ep": to}, device_id_type=pl.DeviceIdType.MESH)
    pl.semaphore_wait(barrier, 3)

    metas = [
        send(meta.at[0], meta.at[1 + i], m_send.at[i], m_recv.at[i], to) for i, to in enumerate((right, left, opp))
    ]
    load_own(0).wait()
    both(0, 0)
    for m in metas:
        m.start()
    both(0, 1)
    for c in range(1, NX):
        load_own(c).start()
    for e in range(NB // 2):
        start_gu(0, e)
    base = (me * per).astype(F32)
    first = lax.broadcasted_iota(jnp.int32, (el, tokens), 0).astype(F32) * cap + base
    line = lax.broadcasted_iota(jnp.int32, (cap, tokens), 0).astype(F32)

    def build(b, _):
        @pl.when(b == 1)
        def _():
            for m in metas:
                m.wait_recv()

        s = jnp.full((el, tokens), -1.0, F32)
        g = jnp.zeros((el, tokens), F32)
        for k in range(top):
            r = meta[b, pl.ds(k, 1)] - first
            ok = jnp.logical_and(r >= 0.0, r < cap)
            s = jnp.where(ok, r, s)
            g = jnp.where(ok, meta[b, pl.ds(top + k, 1)], g)
        acc_u[0, pl.ds(0, el), pl.ds(0, tokens)] = s
        acc_u[1, pl.ds(0, el), pl.ds(0, tokens)] = g

        def lines(e, _):
            eq = acc_u[0, pl.ds(e, 1), pl.ds(0, tokens)] == line
            at = pl.multiple_of(e * cap, 16)
            dmat[b, pl.ds(at, cap)] = jnp.where(eq, 1.0, 0.0).astype(BF)
            w = jnp.where(eq, acc_u[1, pl.ds(e, 1), pl.ds(0, tokens)], 0.0).astype(BF)
            for j in range(tokens // BC):
                zbuf[pl.ds(pl.multiple_of(j * per + e * cap, 16), cap)] = w[:, j * BC : (j + 1) * BC]
            return 0

        lax.fori_loop(0, el, lines, 0, unroll=2)
        for i in range(per // 128):
            for j in range(tokens // BC):
                t = zbuf[pl.ds(j * per + i * 128, 128)]
                wmat[b, pl.ds(j * BC, BC), pl.ds(i * 128, 128)] = t.T

        @pl.when(b == 0)
        def _():
            for direction in range(2):
                own(0, direction, 0).wait_recv()
                forward(0, direction).start()
            for c in range(1, NX):
                load_own(c).wait()
            both(1, 0)
            both(1, 1)
            both(2, 0)

        return 0

    lax.fori_loop(0, n, build, 0)

    def gate_up(c, p, first, last):
        q = c * (2 * el) + 4 * p
        slots = [wait_tile(q + i) for i in range(4)]
        for u in range(2):
            e = 2 * p + u
            z = zbuf[pl.ds(pl.multiple_of(e * rows, 16), rows)]
            for j in range(ff // BC):
                cols = pl.ds(j * BC, BC)
                g = dot(z, wbuf[slots[2 * u], :, cols])
                v = dot(z, wbuf[slots[2 * u + 1], :, cols])
                if not first:
                    g = acc_g[e, :, cols] + g
                    v = acc_u[e, :, cols] + v
                if last:
                    acc_g[e, :, cols] = (g * jax.nn.sigmoid(g) * v).astype(BF).astype(F32)
                else:
                    acc_g[e, :, cols] = g
                    acc_u[e, :, cols] = v
        ahead = 2 * p + NB // 2
        if last:

            @pl.when(ahead < el)
            def _():
                for u in range(2):
                    start_gu(c, ahead + u)

            @pl.when(ahead >= el)
            def _():
                for u in range(4):
                    start_dn(0, 2 * (ahead - el) + u)
        else:
            over = (ahead >= el).astype(jnp.int32)
            for u in range(2):
                start_gu(c + over, ahead + u - over * el)

    def phase1(c, first=False, last=False):
        slot = lax.rem(c, NX)
        if not (first or last):
            service(c + 1, True)
        for direction in range(2):
            own(c, direction, 1).wait_recv()
        for b in range(n):
            if b == 3:
                for direction in range(2):
                    forward(c, direction).wait_recv()
            for i in range(2):
                z = dot(dmat[b, pl.ds(i * (per // 2), per // 2)], xbuf[slot, b]).astype(BF)
                for e in range(el // 2):
                    zbuf[pl.ds((i * (el // 2) + e) * rows + b * cap, cap)] = z[e * cap : (e + 1) * cap]
        for direction in range(2):
            own(c, direction, 0).wait_send()
            own(c, direction, 1).wait_send()
            forward(c, direction).wait_send()

        def free():
            for direction, to in enumerate((left, right)):
                pl.semaphore_signal(
                    credit.at[direction], inc=1, device_id={"ep": to}, device_id_type=pl.DeviceIdType.MESH
                )

        if last:
            free()
        else:
            pl.when(c + NX < nc)(free)
        def body(p, _):
            gate_up(c, p, first, last)
            return 0

        if first:
            service(c + 1, False)
        lax.fori_loop(0, el // 4, body, 0)
        if not last:

            @pl.when(c + NX < nc)
            def _():
                load_own(c + NX).start()

        lax.fori_loop(el // 4, el // 2, body, 0)

    def loop1(c, _):
        phase1(c)
        return 0

    phase1(0, first=True)
    lax.fori_loop(1, nc - 1, loop1, 0)
    phase1(nc - 1, last=True)

    def keep(kind, c, i, value):
        acc_u[2 * c + i, pl.ds(0, half), pl.ds(kind * BC, BC)] = value

    def kept(kind, c, i):
        return acc_u[2 * c + i, pl.ds(0, half), pl.ds(kind * BC, BC)]

    def sl_at(slot, i):
        block = 2 + 2 * slot + i
        return xbuf.at[block // n, lax.rem(block, n)]

    def ro_at(c, i):
        return xbuf.at[2 + c // n, lax.rem(c, n), pl.ds(i * half, half)]

    def put_o(slot, r, value):
        xbuf[0, slot, r] = value

    def send_o(c, i):
        slot = lax.rem(c, 2)
        return send(
            xbuf.at[0, slot, pl.ds(i * half, half)], ro_at(c, i), o_send.at[i, slot], o_recv.at[i, c],
            (left, right)[i],
        )

    def send_l(c, i):
        slot = lax.rem(c, 2)
        return send(
            sl_at(slot, i), last_ref.at[i] if isinstance(c, int) and c == nc - 1 else rl_ref.at[c, i], l_send.at[i, slot], l_recv.at[i, c], (left, right)[i]
        )

    def stage_l(c):
        return pltpu.make_async_copy(rl_ref.at[c], xbuf.at[1, pl.ds(2, 2)], st_sem.at[1])

    def out_y(c):
        return pltpu.make_async_copy(ybuf, y_ref.at[:, pl.ds(c * BC, BC)], y_sem.at[0])

    def out_own(i):
        return pltpu.make_async_copy(
            acc_u.at[2 * (nc - 1) + i, pl.ds(0, half), pl.ds(0, BC)], own_ref.at[pl.ds(i * half, half)], own_sem.at[i]
        )

    def arrive_o(c):
        for i in range(2):
            send_o(c, i).wait_recv()

    def arrive_l(c):
        for i in range(2):
            send_l(c, i).wait_recv()
        stage_l(c).start()

    def pass_on(c):
        slot = lax.rem(c, 2)

        @pl.when(c >= 2)
        def _():
            for i in range(2):
                send_l(c - 2, i).wait_send()

        for i in range(2):
            to = sl_at(slot, i)
            to[pl.ds(i * half, half)] = (kept(1 + i, c, i) + ro_at(c, i)[...].astype(F32)).astype(BF)
            to[pl.ds((1 - i) * half, half)] = kept(1 + i, c, 1 - i).astype(BF)
            send_l(c, i).start()

    def finish(c):
        stage_l(c).wait()

        @pl.when(c >= 1)
        def _():
            out_y(c - 1).wait()

        for i in range(2):
            r = pl.ds(i * half, half)
            ybuf[r] = (kept(0, c, i) + xbuf[1, 2, r].astype(F32) + xbuf[1, 3, r].astype(F32)).astype(BF)
        out_y(c).start()

    def phase2(c, _):
        def down(p, _):
            q = tiles1 + c * el + 4 * p
            slots = [wait_tile(q + i) for i in range(4)]
            for u in range(4):
                e = 4 * p + u
                w = jnp.concatenate([wbuf[slots[u], :, pl.ds(j * BC, BC)] for j in range(ff // BC)], axis=0)
                o = dot(acc_g[e].astype(BF), w).astype(BF)
                for b in range(n):
                    zbuf[pl.ds(pl.multiple_of(b * per + e * cap, 16), cap)] = o[b * cap : (b + 1) * cap]
            r = c * el + 4 * p + NB

            @pl.when(r < nc * el)
            def _():
                for i in range(4):
                    start_dn(r // el, lax.rem(r, el) + i)

            return 0

        lax.fori_loop(0, el // 4, down, 0)

        slot = lax.rem(c, 2)

        @pl.when(c >= 2)
        def _():
            for i in range(2):
                send_o(c - 2, i).wait_send()

        for i in range(2):
            r = pl.ds(i * half, half)
            put_o(slot, r, dot(wmat[3, r], zbuf[pl.ds(3 * per, per)]).astype(BF))
        @pl.when(c == 0)
        def _():
            for i in range(2):
                pl.semaphore_wait(credit.at[i], 1)

        for i in range(2):
            send_o(c, i).start()

        @pl.when(c >= 1)
        def _():
            arrive_o(c - 1)

        @pl.when(c >= 3)
        def _():
            arrive_l(c - 3)

        for kind in range(3):
            for i in range(2):
                keep(kind, c, i, dot(wmat[kind, pl.ds(i * half, half)], zbuf[pl.ds(kind * per, per)]))

        @pl.when(c >= 1)
        def _():
            pass_on(c - 1)

        @pl.when(c >= 3)
        def _():
            finish(c - 3)

        return 0

    lax.fori_loop(0, nc, phase2, 0)
    for i in range(2):
        out_own(i).start()
    arrive_o(nc - 1)
    pass_on(nc - 1)
    for c in (nc - 3, nc - 2):
        arrive_l(c)
        finish(c)
    out_y(nc - 2).wait()
    for i in range(2):
        out_own(i).wait()
        send_l(nc - 1, i).wait_recv()
    for c in (nc - 2, nc - 1):
        for i in range(2):
            send_o(c, i).wait_send()
            send_l(c, i).wait_send()

    for m in metas:
        m.wait_send()


def end_kernel(most_ref, last_ref, own_ref, y_ref, most, last, own, end, in_sem, out_sem, sem):
    tokens, width = most.shape
    lasts = [
        pltpu.make_async_copy(last_ref, last, sem.at[0]),
        pltpu.make_async_copy(own_ref, own, sem.at[1]),
    ]
    rows = [pl.ds(i * (tokens // PIECES), tokens // PIECES) for i in range(PIECES)]
    ins = [pltpu.make_async_copy(most_ref.at[r], most.at[r], in_sem.at[i]) for i, r in enumerate(rows)]
    outs = [pltpu.make_async_copy(most.at[r], y_ref.at[r, pl.ds(0, width)], out_sem.at[i]) for i, r in enumerate(rows)]
    for c in ins + lasts:
        c.start()
    for i, o in zip(ins, outs):
        i.wait()
        o.start()
    for c in lasts:
        c.wait()
    end[...] = (own[...] + last[0].astype(F32) + last[1].astype(F32)).astype(BF)
    final = pltpu.make_async_copy(end, y_ref.at[:, pl.ds(width, end.shape[1])], sem.at[2])
    final.start()
    for o in outs:
        o.wait()
    final.wait()


def solution(mesh):
    n = mesh.shape["ep"]

    def step(x, expert, slot, gate, w_gate, w_up, w_down):
        x, expert, slot, gate = (v[0, 0] for v in (x, expert, slot, gate))
        tokens, d = x.shape
        el, _, ff = w_gate.shape
        top = expert.shape[1]
        cap = 5 * tokens * top // (4 * el * n)
        nc = d // BC
        any_, vmem = pl.BlockSpec(memory_space=pl.ANY), pl.BlockSpec(memory_space=pltpu.VMEM)
        dma = pltpu.SemaphoreType.DMA
        y, _, last, own = pl.pallas_call(
            functools.partial(kernel, n, el, cap),
            out_shape=[
                jax.ShapeDtypeStruct((tokens, d - BC), BF),
                jax.ShapeDtypeStruct((nc - 1, 2, tokens, BC), BF),
                jax.ShapeDtypeStruct((2, tokens, BC), BF),
                jax.ShapeDtypeStruct((tokens, BC), F32),
            ],
            in_specs=[any_, vmem, vmem, vmem, any_, any_, any_],
            out_specs=[any_] * 4,
            scratch_shapes=[
                pltpu.VMEM((el, n * cap, ff), F32),
                pltpu.VMEM((el, n * cap, ff), F32),
                pltpu.VMEM((n, el * cap, tokens), BF),
                pltpu.VMEM((n, tokens, el * cap), BF),
                pltpu.VMEM((NX, n, tokens, BC), BF),
                pltpu.VMEM((n * el * cap, BC), BF),
                pltpu.VMEM((NB, BC, ff), BF),
                pltpu.VMEM((tokens, BC), BF),
                pltpu.VMEM((n, 2 * top, tokens), F32),
                dma((NB,)),
                dma((NX,)),
                dma((6, nc)),
                dma((6, nc)),
                dma((3,)),
                dma((3,)),
                dma((2, 2)),
                dma((2, nc)),
                dma((2, 2)),
                dma((2, nc)),
                dma((2,)),
                dma((1,)),
                dma((2,)),
                pltpu.SemaphoreType.REGULAR((2,)),
            ],
            compiler_params=pltpu.CompilerParams(
                collective_id=0, has_side_effects=True, vmem_limit_bytes=67043328
            ),
        )(x, expert.T, slot.T, gate.T, w_gate, w_up, w_down)
        y = pl.pallas_call(
            end_kernel,
            out_shape=jax.ShapeDtypeStruct((tokens, d), BF),
            in_specs=[any_] * 3,
            out_specs=any_,
            scratch_shapes=[
                pltpu.VMEM((tokens, d - BC), BF),
                pltpu.VMEM((2, tokens, BC), BF),
                pltpu.VMEM((tokens, BC), F32),
                pltpu.VMEM((tokens, BC), BF),
                dma((PIECES,)),
                dma((PIECES,)),
                dma((3,)),
            ],
            compiler_params=pltpu.CompilerParams(vmem_limit_bytes=67043328),
        )(y, last, own)
        return y[None, None]

    token, weight = P("dp", "ep", None, None), P("ep", None, None)
    return jax.shard_map(
        step,
        mesh=mesh,
        in_specs=(token,) * 4 + (weight,) * 3,
        out_specs=token,
        check_vma=False,
    )
```
